256 devices in a mesh: seq: 32 (over y, z), head: 8 (over x, core).
Axes of the slice: x: 4, y: 4, z: 8, core: 2. Of those that a mesh axis runs over, the one named last changes fastest.
Arguments:
- query_rows: bfloat16 [32768, 4096], P('seq', 'head'), may hold values from -6 to 6
- key_rows: bfloat16 [32768, 1024], P('seq', 'head'), may hold values from -6 to 6
- value_rows: bfloat16 [32768, 1024], P('seq', 'head'), may hold values from -6 to 6
- attn_out: bfloat16 [32768, 4096], P('seq', 'head'), may hold values from -4 to 4
- out_grad: bfloat16 [32768, 4096], P(('seq', 'head')), may hold values from -6 to 6
- block_index: int32 [256, 8], P('seq'), may hold values from 0 to 255, as said below
- block_count: int32 [256], P('seq'), may hold values from 1 to 8
Outputs:
- query_grad: bfloat16 [32768, 4096], P('seq', 'head')
- key_grad: bfloat16 [32768, 1024], P('seq', 'head')
- value_grad: bfloat16 [32768, 1024], P('seq', 'head')
The draws below stay inside these ranges and needn't reach their ends.
Inputs may be any that keep to these rules, and one draw needn't show every extreme that they name: `block_index`: row i lists distinct blocks, all at or before block i; its first entry is block i, and blocks i - 1, i - 2 and 0 are listed wherever they exist and differ from i. Entries at or past block_count[i] repeat block i. Counting with repetition the entries of the 8 query blocks of one index of seq that name blocks held by another index, leaving out block 0 and, for the index just below, its last two blocks: at most 1 for any pair of indices, and exactly 1 for some pair in every draw.
All inputs are finite; a program needn't handle non-finite values.
Results may differ from the reference program's by a relative error of at most 0.006.
Values may be sent and summed in bfloat16 or wider, within the bound.
No kernel may reach another device: no remote copies, remote signals or barrier semaphores. Data moves between devices by JAX's collectives and lax.ppermute only.
A program may use at most 64 MiB of HBM per device.

```python
import jax
import jax.numpy as jnp
from jax import lax

HD = 128
HQ = 32
KVH = 8
BLK = 128
NF = 4
MAXB = 8
QB_DEV = 8
TOKENS = 32768
QBLOCKS = 256
CAP = 1
N_SEQ = 32


def draw_query_rows(key, part):
    values = jax.random.normal(jax.random.fold_in(key, 1), (TOKENS, HQ * HD), jnp.float32)
    return jnp.clip(values, -6.0, 6.0).astype(jnp.bfloat16)


def draw_key_rows(key, part):
    values = jax.random.normal(jax.random.fold_in(key, 3), (TOKENS, KVH * HD), jnp.float32)
    return jnp.clip(values, -6.0, 6.0).astype(jnp.bfloat16)


def layout_tables(key):
    base_key = jax.random.fold_in(key, 23)
    devices = jnp.arange(N_SEQ, dtype=jnp.int32)
    permutes = jax.vmap(lambda device: jax.random.permutation(jax.random.fold_in(base_key, device), QB_DEV * NF))(devices)
    shifts = jax.random.randint(jax.random.fold_in(base_key, 101), (N_SEQ, QB_DEV), 0, QB_DEV)
    kept_far = jax.random.randint(jax.random.fold_in(base_key, 102), (N_SEQ, QB_DEV, NF), 0, 4) > 0
    kept_far = kept_far | (devices == N_SEQ - 1)[:, None, None]
    row_ids = jnp.arange(QB_DEV, dtype=jnp.int32)
    slot_ids = jnp.arange(NF, dtype=jnp.int32)
    slot_order = row_ids[:, None] * NF + slot_ids[None, :]
    distance = 1 + permutes[:, slot_order] // CAP
    owner_dev = devices[:, None, None] - distance
    within = (shifts[:, :, None] + slot_ids[None, None, :]) % QB_DEV
    far_block = owner_dev * QB_DEV + within
    query_block = devices[:, None] * QB_DEV + row_ids[None, :]
    far_usable = kept_far & (owner_dev >= 0) & (far_block >= 1) & (far_block <= query_block[..., None] - 3)
    near = jnp.stack([query_block, query_block - 1, query_block - 2, jnp.zeros_like(query_block)], axis=-1)
    near_usable = jnp.stack([query_block >= 0, query_block >= 1, query_block >= 2, query_block >= 3], axis=-1)
    entries = jnp.concatenate([near, far_block], axis=-1)
    usable = jnp.concatenate([near_usable, far_usable], axis=-1)
    width = 4 + NF
    sorter = jnp.argsort((1 - usable.astype(jnp.int32)) * width + jnp.arange(width, dtype=jnp.int32), axis=-1)
    sorted_entries = jnp.take_along_axis(entries, sorter, axis=-1)
    sorted_usable = jnp.take_along_axis(usable, sorter, axis=-1)
    table = jnp.where(sorted_usable, sorted_entries, query_block[..., None]).astype(jnp.int32)
    counted = jnp.sum(usable.astype(jnp.int32), axis=-1)
    return (table.reshape(QBLOCKS, MAXB), counted.reshape(QBLOCKS))


def draw_block_index(key, part):
    return layout_tables(key)[0]


def draw_block_count(key, part):
    return layout_tables(key)[1]


def steps_of(rng, extent, pieces, low, top_value):
    def one(dim, shards_of):
        steps = jax.random.uniform(jax.random.fold_in(jax.random.fold_in(rng, 6), dim), (shards_of,), jnp.float32, low / len(pieces), top_value / len(pieces))
        return jnp.repeat(jnp.exp(steps), extent[dim] // shards_of).reshape((-1,) + (1,) * (len(extent) - dim - 1))

    factor_of = one(*pieces[0])
    for cut in pieces[1:]:
        factor_of = factor_of * one(*cut)
    return factor_of


def bell_draw(rng, shape, scale, reach, cuts=(), kind=jnp.bfloat16):
    level = steps_of(rng, shape, cuts, -0.22, 0.18) if cuts else 1.0
    values = jax.random.normal(rng, shape, jnp.float32) * scale * level
    return jnp.minimum(jnp.maximum(values, -reach), reach).astype(kind)


def setup_inputs(seed: int = 0) -> dict:
    key_of = jax.random.split(jax.random.key(seed), 8)
    query_rows = draw_query_rows(jax.random.fold_in(key_of[7], 71), 0)
    key_rows = draw_key_rows(jax.random.fold_in(key_of[7], 71), 0)
    value_rows = bell_draw(key_of[2], (TOKENS, KVH * HD), 1.0, 6.0, ((0, 32), (1, 8)))
    attn_out = bell_draw(key_of[3], (TOKENS, HQ * HD), 0.5, 4.0, ((0, 32), (1, 8)))
    out_grad = bell_draw(key_of[4], (TOKENS, HQ * HD), 1.0, 6.0, ((0, 256),))
    block_index = draw_block_index(jax.random.fold_in(key_of[7], 71), 0)
    block_count = draw_block_count(jax.random.fold_in(key_of[7], 71), 0)
    return dict(query_rows=query_rows, key_rows=key_rows, value_rows=value_rows, attn_out=attn_out, out_grad=out_grad, block_index=block_index, block_count=block_count)


def reference(query_rows, key_rows, value_rows, attn_out, out_grad, block_index, block_count):
    tokens = query_rows.shape[0]
    qblocks = tokens // BLK
    kv_heads = key_rows.shape[1] // HD
    group_size = query_rows.shape[1] // (kv_heads * HD)
    max_blocks = block_index.shape[1]
    scale_factor = HD ** -0.5
    query_blocks = query_rows.reshape(qblocks, BLK, kv_heads, group_size, HD)
    grad_blocks = out_grad.reshape(qblocks, BLK, kv_heads, group_size, HD)
    out_blocks = attn_out.reshape(qblocks, BLK, kv_heads, group_size, HD)
    key_blocks = key_rows.reshape(qblocks, BLK, kv_heads, HD)
    value_blocks = value_rows.reshape(qblocks, BLK, kv_heads, HD)
    offsets = jnp.arange(BLK, dtype=jnp.int32)

    def one_block(carry, inputs):
        key_acc, value_acc = carry
        row_number, query_tile, grad_tile, out_tile, tile_index, tile_count = inputs
        key_tile = key_blocks[tile_index].astype(jnp.float32)
        value_tile = value_blocks[tile_index].astype(jnp.float32)
        query_wide = query_tile.astype(jnp.float32)
        grad_wide = grad_tile.astype(jnp.float32)
        scores = jnp.einsum("rgqd,mcgd->gqrmc", query_wide, key_tile) * scale_factor
        query_pos = row_number * BLK + offsets
        key_pos = tile_index[:, None] * BLK + offsets[None, :]
        is_live = jnp.arange(max_blocks, dtype=jnp.int32)[:, None] < tile_count
        allowed = is_live[None] & (key_pos[None] <= query_pos[:, None, None])
        masked = jnp.where(allowed, scores, -jnp.inf)
        row_top = jnp.max(masked, axis=(3, 4), keepdims=True)
        exponent = jnp.exp(masked - row_top)
        probs_full = exponent / jnp.sum(exponent, axis=(3, 4), keepdims=True)
        probs_low = lax.optimization_barrier(probs_full.astype(jnp.bfloat16)).astype(jnp.float32)
        dprobs = jnp.einsum("rgqd,mcgd->gqrmc", grad_wide, value_tile)
        out_dot = jnp.sum(grad_wide * out_tile.astype(jnp.float32), axis=-1)
        out_dot = jnp.transpose(out_dot, (1, 2, 0))[..., None, None]
        dscores = lax.optimization_barrier((probs_full * (dprobs - out_dot)).astype(jnp.bfloat16)).astype(jnp.float32)
        query_grad_tile = jnp.einsum("gqrmc,mcgd->rgqd", dscores, key_tile) * scale_factor
        key_part = jnp.einsum("gqrmc,rgqd->mcgd", dscores, query_wide) * scale_factor
        value_part = jnp.einsum("gqrmc,rgqd->mcgd", probs_low, grad_wide)
        key_acc = key_acc.at[tile_index].add(key_part)
        value_acc = value_acc.at[tile_index].add(value_part)
        return (key_acc, value_acc), query_grad_tile.reshape(BLK, -1).astype(jnp.bfloat16)

    zeros_acc = jnp.zeros((qblocks, BLK, kv_heads, HD), jnp.float32)
    inputs = (jnp.arange(qblocks, dtype=jnp.int32), query_blocks, grad_blocks, out_blocks, block_index, block_count)
    (key_acc, value_acc), query_grad = lax.scan(one_block, (zeros_acc, zeros_acc), inputs)
    query_grad = query_grad.reshape(tokens, -1)
    key_grad = key_acc.reshape(tokens, -1).astype(jnp.bfloat16)
    value_grad = value_acc.reshape(tokens, -1).astype(jnp.bfloat16)
    return query_grad, key_grad, value_grad
```

```python
import functools

import jax
import jax.numpy as jnp
from jax import lax
from jax.experimental import pallas as pl
from jax.experimental.pallas import tpu as pltpu
from jax.sharding import PartitionSpec as P

HD = 128
GROUP = 4
BLK = 128
SCALE = HD ** (-0.5)
LOG2E = 1.4426950408889634
F32 = jnp.float32
BF16 = jnp.bfloat16


def dot(a, b, dims):
    return lax.dot_general(a, b, (dims, ((), ())), preferred_element_type=F32)


def serve_kernel(asked, k_ref, v_ref, out_ref):
    def step(d, carry):
        w = asked[d]
        out_ref[d, :, :HD] = k_ref[w]
        out_ref[d, :, HD:] = v_ref[w]
        return carry

    lax.fori_loop(0, out_ref.shape[0], step, 0)


def serve(asked, keys, values):
    count = asked.shape[0]
    return pl.pallas_call(
        serve_kernel,
        out_shape=jax.ShapeDtypeStruct((count, BLK, 2 * HD), BF16),
        grid_spec=pltpu.PrefetchScalarGridSpec(
            num_scalar_prefetch=1,
            grid=(1,),
            in_specs=[
                pl.BlockSpec(keys.shape, lambda i, *_: (0, 0, 0)),
                pl.BlockSpec(values.shape, lambda i, *_: (0, 0, 0)),
            ],
            out_specs=pl.BlockSpec((count, BLK, 2 * HD), lambda i, *_: (0, 0, 0)),
        ),
        name="serve",
    )(asked, keys, values)


def attn_kernel(
    qblocks, max_blocks, far_count,
    pos, live, order,
    q_ref, do_ref, o_ref, k_ref, v_ref, prev_ref, first_ref, far_ref,
    dq_ref, own_ref, dprev_ref, dfirst_ref, dfar_ref,
    k_all, v_all, acc, qs, ds, kg, vg, s_buf, dp_buf, pt, dst,
):
    row = pl.program_id(0)
    slots = qblocks + 3 + far_count
    keys = max_blocks * BLK
    width = GROUP * BLK

    @pl.when(row == 0)
    def _():
        k_all[:qblocks] = k_ref[...]
        v_all[:qblocks] = v_ref[...]
        for i in range(2):
            k_all[qblocks + i] = prev_ref[i, :, :HD]
            v_all[qblocks + i] = prev_ref[i, :, HD:]
        k_all[qblocks + 2] = first_ref[:, :HD]
        v_all[qblocks + 2] = first_ref[:, HD:]

        def copy_far(d, carry):
            k_all[qblocks + 3 + d] = far_ref[d, :, :HD]
            v_all[qblocks + 3 + d] = far_ref[d, :, HD:]
            return carry

        lax.fori_loop(0, far_count, copy_far, 0)

        def clear(d, carry):
            acc[d] = jnp.zeros((BLK, 2 * HD), F32)
            return carry

        lax.fori_loop(0, slots, clear, 0)

    for g in range(GROUP):
        cols = slice(g * HD, (g + 1) * HD)
        qs[g * BLK:(g + 1) * BLK] = q_ref[:, cols]
        ds[g * BLK:(g + 1) * BLK] = do_ref[0, :, cols]
    for e in range(max_blocks):
        p = pos[row * max_blocks + e]
        kg[e * BLK:(e + 1) * BLK] = k_all[p]
        vg[e * BLK:(e + 1) * BLK] = v_all[p]

    s_buf[...] = dot(kg[...], qs[...], ((1,), (1,)))
    dp_buf[...] = dot(vg[...], ds[...], ((1,), (1,)))

    ones = jnp.ones((8, 2 * HD), BF16)
    parts = []
    for g in range(GROUP):
        cols = slice(g * HD, (g + 1) * HD)
        prod = do_ref[0, :, cols].astype(F32) * o_ref[:, cols].astype(F32)
        high = prod.astype(BF16)
        low = (prod - high.astype(F32)).astype(BF16)
        both = jnp.concatenate([high, low], axis=1)
        parts.append(dot(ones, both, ((1,), (1,))))
    out_dot = jnp.concatenate(parts, axis=1)[0:1]

    key_at = lax.broadcasted_iota(jnp.int32, (BLK, width), 0)
    query_at = lax.broadcasted_iota(jnp.int32, (BLK, width), 1) % BLK
    diagonal = jnp.where(key_at <= query_at, s_buf[:BLK], -jnp.inf)
    s_buf[:BLK] = diagonal
    top = None
    for e in range(max_blocks):
        part = s_buf[e * BLK:(e + 1) * BLK].reshape(BLK // 8, 8, width).max(axis=0)
        if e:
            part = jnp.where(live[row * max_blocks + e] > 0, part, -jnp.inf)
        top = part if top is None else jnp.maximum(top, part)
    top = top.max(axis=0, keepdims=True)
    shift = top * (SCALE * LOG2E)
    total = None
    for e in range(max_blocks):
        rows = slice(e * BLK, (e + 1) * BLK)
        if e:
            this = jnp.where(live[row * max_blocks + e] > 0, shift, jnp.inf)
        else:
            this = shift
        value = jnp.exp2(s_buf[rows] * (SCALE * LOG2E) - this)
        s_buf[rows] = value
        part = value.reshape(BLK // 8, 8, width).sum(axis=0)
        total = part if total is None else total + part
    inverse = 1.0 / total.sum(axis=0, keepdims=True)
    for e in range(max_blocks):
        rows = slice(e * BLK, (e + 1) * BLK)
        probs = s_buf[rows] * inverse
        pt[rows] = probs.astype(BF16)
        dst[rows] = (probs * (dp_buf[rows] - out_dot)).astype(BF16)

    dv = dot(pt[...], ds[...], ((1,), (0,)))
    dk = dot(dst[...], qs[...], ((1,), (0,))) * SCALE
    for e in range(max_blocks):
        rows = slice(e * BLK, (e + 1) * BLK)
        p = pos[row * max_blocks + e]
        acc[p, :, :HD] += dk[rows]
        acc[p, :, HD:] += dv[rows]
    dqt = dot(kg[...], dst[...], ((0,), (0,))) * SCALE
    for g in range(GROUP):
        cols = slice(g * HD, (g + 1) * HD)
        dq_ref[:, cols] = dqt[:, cols].T.astype(BF16)

    @pl.when(row == qblocks - 1)
    def _():
        own_ref[...] = acc[:qblocks]
        dprev_ref[...] = acc[qblocks:qblocks + 2].astype(BF16)
        dfirst_ref[...] = acc[qblocks + 2]

        def put(d, carry):
            dfar_ref[d] = acc[qblocks + 3 + d].astype(BF16)
            return carry

        lax.fori_loop(0, far_count, put, 0)


def attention(pos, live, order, q, do, o, keys, values, prev, first, far):
    qblocks, far_count = keys.shape[0], far.shape[0]
    max_blocks = pos.shape[0] // qblocks
    slots = qblocks + 3 + far_count
    nkeys = max_blocks * BLK
    width = GROUP * BLK

    def whole(shape):
        return pl.BlockSpec(shape, lambda i, *_: (0,) * len(shape))

    out_shapes = (
        jax.ShapeDtypeStruct(q.shape, BF16),
        jax.ShapeDtypeStruct((qblocks, BLK, 2 * HD), F32),
        jax.ShapeDtypeStruct((2, BLK, 2 * HD), BF16),
        jax.ShapeDtypeStruct((BLK, 2 * HD), F32),
        jax.ShapeDtypeStruct((far_count, BLK, 2 * HD), BF16),
    )
    rows = pl.BlockSpec((BLK, width), lambda i, *_: (i, 0))
    return pl.pallas_call(
        functools.partial(attn_kernel, qblocks, max_blocks, far_count),
        out_shape=out_shapes,
        grid_spec=pltpu.PrefetchScalarGridSpec(
            num_scalar_prefetch=3,
            grid=(qblocks,),
            in_specs=[
                rows,
                pl.BlockSpec((1, BLK, width), lambda i, pos, live, order: (order[i], 0, 0)),
                rows,
                whole(keys.shape), whole(values.shape), whole(prev.shape),
                whole(first.shape), whole(far.shape),
            ],
            out_specs=[rows] + [whole(s.shape) for s in out_shapes[1:]],
            scratch_shapes=[
                pltpu.VMEM((slots, BLK, HD), BF16),
                pltpu.VMEM((slots, BLK, HD), BF16),
                pltpu.VMEM((slots, BLK, 2 * HD), F32),
                pltpu.VMEM((width, HD), BF16),
                pltpu.VMEM((width, HD), BF16),
                pltpu.VMEM((nkeys, HD), BF16),
                pltpu.VMEM((nkeys, HD), BF16),
                pltpu.VMEM((nkeys, width), F32),
                pltpu.VMEM((nkeys, width), F32),
                pltpu.VMEM((nkeys, width), BF16),
                pltpu.VMEM((nkeys, width), BF16),
            ],
        ),
        compiler_params=pltpu.CompilerParams(dimension_semantics=("arbitrary",)),
        cost_estimate=pl.CostEstimate(
            flops=10 * nkeys * width * HD * qblocks, bytes_accessed=16 << 20, transcendentals=0
        ),
        name="attention",
    )(pos, live, order, q, do, o, keys, values, prev, first, far)


def finish_kernel(
    qblocks, far_count, asked, is_root,
    own_ref, prev_ref, first_ref, far_ref, dk_ref, dv_ref, acc,
):
    acc[...] = own_ref[...]
    acc[qblocks - 2:] += prev_ref[...].astype(F32)

    @pl.when(is_root[0] > 0)
    def _():
        acc[0] += first_ref[...]

    def step(d, carry):
        w = asked[d]

        @pl.when(w > 0)
        def _():
            acc[w - 1] += far_ref[d].astype(F32)

        return carry

    lax.fori_loop(0, far_count, step, 0)
    for b in range(qblocks):
        dk_ref[b * BLK:(b + 1) * BLK] = acc[b, :, :HD].astype(BF16)
        dv_ref[b * BLK:(b + 1) * BLK] = acc[b, :, HD:].astype(BF16)


def finish(asked, is_root, own, prev, first, far):
    qblocks, far_count = own.shape[0], far.shape[0]

    def whole(shape):
        return pl.BlockSpec(shape, lambda i, *_: (0,) * len(shape))

    out = jax.ShapeDtypeStruct((qblocks * BLK, HD), BF16)
    return pl.pallas_call(
        functools.partial(finish_kernel, qblocks, far_count),
        out_shape=(out, out),
        grid_spec=pltpu.PrefetchScalarGridSpec(
            num_scalar_prefetch=2,
            grid=(1,),
            in_specs=[whole(own.shape), whole(prev.shape), whole(first.shape), whole(far.shape)],
            out_specs=[whole(out.shape), whole(out.shape)],
            scratch_shapes=[pltpu.VMEM(own.shape, F32)],
        ),
        name="finish",
    )(asked, is_root, own, prev, first, far)


def local(query_rows, key_rows, value_rows, attn_out, out_grad, block_index, block_count):
    count = lax.axis_size("seq")
    me = lax.axis_index("seq")
    heads = lax.axis_size("head")
    my_head = lax.axis_index("head")
    qblocks = key_rows.shape[0] // BLK
    max_blocks = block_index.shape[1]
    keys = key_rows.reshape(qblocks, BLK, HD)
    values = value_rows.reshape(qblocks, BLK, HD)

    owner = block_index // qblocks
    within = block_index % qblocks
    live = jnp.arange(max_blocks, dtype=jnp.int32)[None, :] < block_count[:, None]
    is_local = owner == me
    is_prev = (owner == me - 1) & (within >= qblocks - 2)
    is_first = (block_index == 0) & ~is_local & ~is_prev
    is_far = live & ~is_local & ~is_prev & ~is_first
    position = jnp.where(
        is_local,
        within,
        jnp.where(
            is_prev, within + 2, jnp.where(is_first, qblocks + 2, qblocks + 3 + owner)
        ),
    ).reshape(-1)
    devices = jnp.arange(count, dtype=jnp.int32)[:, None]
    hit = is_far.reshape(1, -1) & (owner.reshape(1, -1) == devices)
    request = jnp.max(jnp.where(hit, within.reshape(1, -1) + 1, 0), axis=1)

    asked = lax.all_to_all(
        request[:, None], "seq", split_axis=0, concat_axis=0, tiled=True
    ).reshape(-1)
    served = serve(jnp.maximum(asked - 1, 0), keys, values)
    far = lax.all_to_all(served, "seq", split_axis=0, concat_axis=0, tiled=True)

    tail = jnp.concatenate([keys[qblocks - 2:], values[qblocks - 2:]], axis=-1)
    prev = lax.ppermute(tail, "seq", [(s, s + 1) for s in range(count - 1)])

    first = jnp.concatenate([keys[0], values[0]], axis=-1)
    step = count // 2
    while step:
        got = lax.ppermute(
            first, "seq", [(s, s + step) for s in range(0, count, 2 * step)]
        )
        first = jnp.where(me % (2 * step) == step, got, first)
        step //= 2

    width = out_grad.shape[1] // heads
    pieces = []
    for k in range(heads):
        piece = lax.dynamic_slice_in_dim(out_grad, ((my_head + k) % heads) * width, width, 1)
        if k:
            piece = lax.ppermute(piece, "head", [(h, (h + k) % heads) for h in range(heads)])
        pieces.append(piece)
    grads = jnp.stack(pieces)
    order = (my_head - jnp.arange(qblocks, dtype=jnp.int32)) % heads

    dq, own, dprev, dfirst, dfar = attention(
        position, live.astype(jnp.int32).reshape(-1), order,
        query_rows, grads, attn_out, keys, values, prev, first, far,
    )

    far_back = lax.all_to_all(dfar, "seq", split_axis=0, concat_axis=0, tiled=True)
    prev_back = lax.ppermute(dprev, "seq", [(s + 1, s) for s in range(count - 1)])
    step = 1
    while step < count:
        got = lax.ppermute(
            dfirst, "seq", [(s + step, s) for s in range(0, count, 2 * step)]
        )
        dfirst = dfirst + got
        step *= 2
    root = (me == 0).astype(jnp.int32).reshape(1)
    dk, dv = finish(asked, root, own, prev_back, dfirst, far_back)
    return dq, dk, dv


def solution(mesh):
    return jax.shard_map(
        local,
        mesh=mesh,
        in_specs=(
            P("seq", "head"),
            P("seq", "head"),
            P("seq", "head"),
            P("seq", "head"),
            P(("seq", "head"), None),
            P("seq", None),
            P("seq"),
        ),
        out_specs=(P("seq", "head"), P("seq", "head"), P("seq", "head")),
        check_vma=False,
    )
```

```python
import functools

import jax
import jax.numpy as jnp
from jax import lax
from jax.experimental import pallas as pl
from jax.experimental.pallas import tpu as pltpu
from jax.sharding import PartitionSpec as P

HD = 128
GROUP = 4
BLK = 128
SCALE = HD ** (-0.5)
LOG2E = 1.4426950408889634
F32 = jnp.float32
BF16 = jnp.bfloat16


def dot(a, b, dims):
    return lax.dot_general(a, b, (dims, ((), ())), preferred_element_type=F32)


def serve_kernel(asked, last, k_ref, v_ref, first_ref, out_ref):
    def step(d, carry):
        w = jnp.maximum(asked[d] - 1, 0)
        out_ref[d, :, :HD] = k_ref[w]
        out_ref[d, :, HD:] = v_ref[w]
        return carry

    def spread(d, carry):
        out_ref[d] = first_ref[...]
        return carry

    @pl.when(last[0] == 0)
    def _():
        lax.fori_loop(0, out_ref.shape[0], step, 0)

    @pl.when(last[0] != 0)
    def _():
        lax.fori_loop(0, out_ref.shape[0], spread, 0)


def whole(shape):
    return pl.BlockSpec(shape, lambda i, *_: (0,) * len(shape))


def serve(asked, last, keys, values, first):
    count = asked.shape[0]
    return pl.pallas_call(
        serve_kernel,
        out_shape=jax.ShapeDtypeStruct((count, BLK, 2 * HD), BF16),
        grid_spec=pltpu.PrefetchScalarGridSpec(
            num_scalar_prefetch=2,
            grid=(1,),
            in_specs=[whole(keys.shape), whole(values.shape), whole(first.shape)],
            out_specs=whole((count, BLK, 2 * HD)),
        ),
        name="serve",
    )(asked, last, keys, values, first)


def attn_kernel(
    qblocks, max_blocks, far_count,
    pos, live, order,
    q_ref, do_ref, o_ref, k_ref, v_ref, prev_ref, far_ref,
    dq_ref, own_ref, dprev_ref, dfar_ref,
    kv_all, acc, qs, ds, kg, vg, s_buf, dp_buf, pt, dst, sems,
):
    row = pl.program_id(0)
    base = qblocks + 2
    slots = base + far_count
    width = GROUP * BLK

    @pl.when(row == 0)
    def _():
        copies = [
            pltpu.make_async_copy(far_ref, kv_all.at[base:], sems.at[0]),
            pltpu.make_async_copy(prev_ref, kv_all.at[qblocks:base], sems.at[1]),
            pltpu.make_async_copy(k_ref, kv_all.at[:qblocks, :, :HD], sems.at[2]),
            pltpu.make_async_copy(v_ref, kv_all.at[:qblocks, :, HD:], sems.at[3]),
        ]
        for copy in copies:
            copy.start()

        def clear(d, carry):
            acc[d] = jnp.zeros((BLK, 2 * HD), F32)
            return carry

        lax.fori_loop(0, slots, clear, 0)
        for copy in copies:
            copy.wait()

    for g in range(GROUP):
        cols = slice(g * HD, (g + 1) * HD)
        qs[g * BLK:(g + 1) * BLK] = q_ref[:, cols]
        ds[g * BLK:(g + 1) * BLK] = do_ref[0, :, cols]
    for e in range(max_blocks):
        p = pos[row * max_blocks + e]
        kg[e * BLK:(e + 1) * BLK] = kv_all[p, :, :HD]
        vg[e * BLK:(e + 1) * BLK] = kv_all[p, :, HD:]

    s_buf[...] = dot(kg[...], qs[...], ((1,), (1,)))
    dp_buf[...] = dot(vg[...], ds[...], ((1,), (1,)))

    ones = jnp.ones((8, 2 * HD), BF16)
    parts = []
    for g in range(GROUP):
        cols = slice(g * HD, (g + 1) * HD)
        prod = do_ref[0, :, cols].astype(F32) * o_ref[:, cols].astype(F32)
        high = prod.astype(BF16)
        low = (prod - high.astype(F32)).astype(BF16)
        both = jnp.concatenate([high, low], axis=1)
        parts.append(dot(ones, both, ((1,), (1,))))
    out_dot = jnp.concatenate(parts, axis=1)[0:1]

    key_at = lax.broadcasted_iota(jnp.int32, (BLK, width), 0)
    query_at = lax.broadcasted_iota(jnp.int32, (BLK, width), 1) % BLK
    diagonal = jnp.where(key_at <= query_at, s_buf[:BLK], -jnp.inf)
    s_buf[:BLK] = diagonal
    top = None
    for e in range(max_blocks):
        part = s_buf[e * BLK:(e + 1) * BLK].reshape(BLK // 8, 8, width).max(axis=0)
        if e:
            part = jnp.where(live[row * max_blocks + e] > 0, part, -jnp.inf)
        top = part if top is None else jnp.maximum(top, part)
    top = top.max(axis=0, keepdims=True)
    shift = top * (SCALE * LOG2E)
    total = None
    for e in range(max_blocks):
        rows = slice(e * BLK, (e + 1) * BLK)
        if e:
            this = jnp.where(live[row * max_blocks + e] > 0, shift, jnp.inf)
        else:
            this = shift
        value = jnp.exp2(s_buf[rows] * (SCALE * LOG2E) - this)
        s_buf[rows] = value
        part = value.reshape(BLK // 8, 8, width).sum(axis=0)
        total = part if total is None else total + part
    inverse = 1.0 / total.sum(axis=0, keepdims=True)
    for e in range(max_blocks):
        rows = slice(e * BLK, (e + 1) * BLK)
        probs = s_buf[rows] * inverse
        pt[rows] = probs.astype(BF16)
        dst[rows] = (probs * (dp_buf[rows] - out_dot)).astype(BF16)

    dv = dot(pt[...], ds[...], ((1,), (0,)))
    dk = dot(dst[...], qs[...], ((1,), (0,))) * SCALE
    for e in range(max_blocks):
        rows = slice(e * BLK, (e + 1) * BLK)
        p = pos[row * max_blocks + e]
        acc[p, :, :HD] += dk[rows]
        acc[p, :, HD:] += dv[rows]
    dqt = dot(kg[...], dst[...], ((0,), (0,))) * SCALE
    for g in range(GROUP):
        cols = slice(g * HD, (g + 1) * HD)
        dq_ref[:, cols] = dqt[:, cols].T.astype(BF16)

    @pl.when(row == qblocks - 1)
    def _():
        own_ref[...] = acc[:qblocks]
        dprev_ref[...] = acc[qblocks:base].astype(BF16)

        def put(d, carry):
            dfar_ref[d] = acc[base + d].astype(BF16)
            return carry

        lax.fori_loop(0, far_count, put, 0)


def attention(pos, live, order, q, do, o, keys, values, prev, far):
    qblocks, far_count = keys.shape[0], far.shape[0]
    max_blocks = pos.shape[0] // qblocks
    slots = qblocks + 2 + far_count
    nkeys = max_blocks * BLK
    width = GROUP * BLK
    out_shapes = (
        jax.ShapeDtypeStruct(q.shape, BF16),
        jax.ShapeDtypeStruct((qblocks, BLK, 2 * HD), F32),
        jax.ShapeDtypeStruct((2, BLK, 2 * HD), BF16),
        jax.ShapeDtypeStruct((far_count, BLK, 2 * HD), BF16),
    )
    rows = pl.BlockSpec((BLK, width), lambda i, *_: (i, 0))
    anywhere = pl.BlockSpec(memory_space=pl.ANY)
    return pl.pallas_call(
        functools.partial(attn_kernel, qblocks, max_blocks, far_count),
        out_shape=out_shapes,
        grid_spec=pltpu.PrefetchScalarGridSpec(
            num_scalar_prefetch=3,
            grid=(qblocks,),
            in_specs=[
                rows,
                pl.BlockSpec((1, BLK, width), lambda i, pos, live, order: (order[i], 0, 0)),
                rows,
                anywhere, anywhere, anywhere, anywhere,
            ],
            out_specs=[rows] + [whole(s.shape) for s in out_shapes[1:]],
            scratch_shapes=[
                pltpu.VMEM((slots, BLK, 2 * HD), BF16),
                pltpu.VMEM((slots, BLK, 2 * HD), F32),
                pltpu.VMEM((width, HD), BF16),
                pltpu.VMEM((width, HD), BF16),
                pltpu.VMEM((nkeys, HD), BF16),
                pltpu.VMEM((nkeys, HD), BF16),
                pltpu.VMEM((nkeys, width), F32),
                pltpu.VMEM((nkeys, width), F32),
                pltpu.VMEM((nkeys, width), BF16),
                pltpu.VMEM((nkeys, width), BF16),
                pltpu.SemaphoreType.DMA((4,)),
            ],
        ),
        compiler_params=pltpu.CompilerParams(dimension_semantics=("arbitrary",)),
        cost_estimate=pl.CostEstimate(
            flops=10 * nkeys * width * HD * qblocks, bytes_accessed=16 << 20, transcendentals=0
        ),
        name="attention",
    )(pos, live, order, q, do, o, keys, values, prev, far)


def root_sum_kernel(last, far_ref, out_ref, buf, sem):
    @pl.when(last[0] != 0)
    def _():
        copy = pltpu.make_async_copy(far_ref, buf, sem)
        copy.start()
        copy.wait()

        def rows(r, carry):
            at = pl.ds(pl.multiple_of(r * 16, 16), 16)
            total = buf[0, at, :].astype(F32)
            for d in range(1, buf.shape[0]):
                total = total + buf[d, at, :].astype(F32)
            out_ref[at, :] = total
            return carry

        lax.fori_loop(0, BLK // 16, rows, 0)


def root_sum(last, far):
    return pl.pallas_call(
        root_sum_kernel,
        out_shape=jax.ShapeDtypeStruct(far.shape[1:], F32),
        grid_spec=pltpu.PrefetchScalarGridSpec(
            num_scalar_prefetch=1,
            grid=(1,),
            in_specs=[pl.BlockSpec(memory_space=pl.ANY)],
            out_specs=whole(far.shape[1:]),
            scratch_shapes=[pltpu.VMEM(far.shape, BF16), pltpu.SemaphoreType.DMA],
        ),
        name="root_sum",
    )(last, far)


def finish_kernel(
    qblocks, far_count, asked, own_ref, prev_ref, far_ref, dk_ref, dv_ref, zero_ref, acc,
):
    acc[...] = own_ref[...]
    acc[qblocks - 2:] += prev_ref[...].astype(F32)

    def step(d, carry):
        w = asked[d]

        @pl.when(w > 0)
        def _():
            acc[w - 1] += far_ref[d].astype(F32)

        return carry

    lax.fori_loop(0, far_count, step, 0)
    zero_ref[...] = acc[0]
    for b in range(qblocks):
        dk_ref[b * BLK:(b + 1) * BLK] = acc[b, :, :HD].astype(BF16)
        dv_ref[b * BLK:(b + 1) * BLK] = acc[b, :, HD:].astype(BF16)


def finish(asked, own, prev, far):
    qblocks, far_count = own.shape[0], far.shape[0]
    out = jax.ShapeDtypeStruct((qblocks * BLK, HD), BF16)
    zero = jax.ShapeDtypeStruct((BLK, 2 * HD), F32)
    return pl.pallas_call(
        functools.partial(finish_kernel, qblocks, far_count),
        out_shape=(out, out, zero),
        grid_spec=pltpu.PrefetchScalarGridSpec(
            num_scalar_prefetch=1,
            grid=(1,),
            in_specs=[whole(own.shape), whole(prev.shape), whole(far.shape)],
            out_specs=[whole(out.shape), whole(out.shape), whole(zero.shape)],
            scratch_shapes=[pltpu.VMEM(own.shape, F32)],
        ),
        cost_estimate=pl.CostEstimate(
            flops=1 << 30, bytes_accessed=8 << 20, transcendentals=0
        ),
        name="finish",
    )(asked, own, prev, far)


def add_first_kernel(is_root, first_ref, zero_ref, dk_in, dv_in, dk_ref, dv_ref):
    del dk_in, dv_in
    extra = jnp.where(is_root[0] != 0, first_ref[...], 0.0)
    total = zero_ref[...] + extra
    dk_ref[...] = total[:, :HD].astype(BF16)
    dv_ref[...] = total[:, HD:].astype(BF16)


def add_first(is_root, first, zero, dk, dv):
    block = pl.BlockSpec((BLK, HD), lambda i, *_: (0, 0))
    anywhere = pl.BlockSpec(memory_space=pl.ANY)
    return pl.pallas_call(
        add_first_kernel,
        out_shape=(
            jax.ShapeDtypeStruct(dk.shape, BF16), jax.ShapeDtypeStruct(dv.shape, BF16)
        ),
        grid_spec=pltpu.PrefetchScalarGridSpec(
            num_scalar_prefetch=1,
            grid=(1,),
            in_specs=[whole(first.shape), whole(zero.shape), anywhere, anywhere],
            out_specs=[block, block],
        ),
        input_output_aliases={3: 0, 4: 1},
        name="add_first",
    )(is_root, first, zero, dk, dv)


def local(query_rows, key_rows, value_rows, attn_out, out_grad, block_index, block_count):
    count = lax.axis_size("seq")
    me = lax.axis_index("seq")
    heads = lax.axis_size("head")
    my_head = lax.axis_index("head")
    qblocks = key_rows.shape[0] // BLK
    max_blocks = block_index.shape[1]
    keys = key_rows.reshape(qblocks, BLK, HD)
    values = value_rows.reshape(qblocks, BLK, HD)

    owner = block_index // qblocks
    within = block_index % qblocks
    live = jnp.arange(max_blocks, dtype=jnp.int32)[None, :] < block_count[:, None]
    is_local = owner == me
    is_prev = (owner == me - 1) & (within >= qblocks - 2)
    is_first = (block_index == 0) & ~is_local & ~is_prev
    is_far = live & ~is_local & ~is_prev & ~is_first
    position = jnp.where(
        is_local,
        within,
        jnp.where(
            is_prev,
            within + 2,
            qblocks + 2 + jnp.where(is_first, count - 1, owner),
        ),
    ).reshape(-1)
    devices = jnp.arange(count, dtype=jnp.int32)[:, None]
    hit = is_far.reshape(1, -1) & (owner.reshape(1, -1) == devices)
    request = jnp.max(jnp.where(hit, within.reshape(1, -1) + 1, 0), axis=1)

    last = (me == count - 1).astype(jnp.int32).reshape(1)
    first = jnp.concatenate([keys[0], values[0]], axis=-1)
    first = lax.ppermute(first, "seq", [(0, count - 1)])
    tail = jnp.concatenate([keys[qblocks - 2:], values[qblocks - 2:]], axis=-1)
    prev = lax.ppermute(tail, "seq", [(s, s + 1) for s in range(count - 1)])

    asked = lax.all_to_all(
        request[:, None], "seq", split_axis=0, concat_axis=0, tiled=True
    ).reshape(-1)
    asked, first, prev = lax.optimization_barrier((asked, first, prev))
    served = serve(asked, last, keys, values, first)
    far = lax.all_to_all(served, "seq", split_axis=0, concat_axis=0, tiled=True)

    width = out_grad.shape[1] // heads
    pieces = []
    for k in range(heads):
        piece = lax.dynamic_slice_in_dim(out_grad, ((my_head + k) % heads) * width, width, 1)
        if k:
            piece = lax.ppermute(piece, "head", [(h, (h + k) % heads) for h in range(heads)])
        pieces.append(piece)
    grads = jnp.stack(pieces)
    order = (my_head - jnp.arange(qblocks, dtype=jnp.int32)) % heads

    dq, own, dprev, dfar = attention(
        position, live.astype(jnp.int32).reshape(-1), order,
        query_rows, grads, attn_out, keys, values, prev, far,
    )

    prev_back = lax.ppermute(dprev, "seq", [(s + 1, s) for s in range(count - 1)])
    far_back = lax.all_to_all(dfar, "seq", split_axis=0, concat_axis=0, tiled=True)
    first_back = lax.ppermute(root_sum(last, far_back), "seq", [(count - 1, 0)])
    dk, dv, zero = finish(asked, own, prev_back, far_back)
    root = (me == 0).astype(jnp.int32).reshape(1)
    dk, dv = add_first(root, first_back, zero, dk, dv)
    return dq, dk, dv


def solution(mesh):
    return jax.shard_map(
        local,
        mesh=mesh,
        in_specs=(
            P("seq", "head"),
            P("seq", "head"),
            P("seq", "head"),
            P("seq", "head"),
            P(("seq", "head"), None),
            P("seq", None),
            P("seq"),
        ),
        out_specs=(P("seq", "head"), P("seq", "head"), P("seq", "head")),
        check_vma=False,
    )
```

```python
import functools

import jax
import jax.numpy as jnp
from jax import lax
from jax.experimental import pallas as pl
from jax.experimental.pallas import tpu as pltpu
from jax.sharding import PartitionSpec as P


HD = 128
GROUP = 4
BLK = 128
SCALE = HD ** (-0.5)
LOG2E = 1.4426950408889634
F32 = jnp.float32
BF16 = jnp.bfloat16


def dot(a, b, dims):
    return lax.dot_general(a, b, (dims, ((), ())), preferred_element_type=F32)


def whole(shape):
    return pl.BlockSpec(shape, lambda i, *_: (0,) * len(shape))


def prepare_kernel(
    count, me, index_ref, live_count_ref, k_first, v_first, k_tail, v_tail,
    request_ref, pos_ref, live_ref, first_ref, tail_ref,
):
    qblocks, max_blocks = index_ref.shape
    mine = me[0]
    for d in range(count):
        request_ref[d, 0, 0] = 0
    for r in range(qblocks):
        for e in range(max_blocks):
            block = index_ref[r, e]
            owner = block // qblocks
            within = block % qblocks
            live = e < live_count_ref[r]
            is_local = owner == mine
            is_prev = (owner == mine - 1) & (within >= qblocks - 2)
            is_first = (block == 0) & ~is_local & ~is_prev
            is_far = live & ~is_local & ~is_prev & ~is_first
            slot = jnp.where(is_first, count - 1, owner) + (qblocks + 2)
            slot = jnp.where(is_prev, within + 2, slot)
            pos_ref[r * max_blocks + e] = jnp.where(is_local, within, slot)
            live_ref[r * max_blocks + e] = live.astype(jnp.int32)
            target = jnp.where(is_far, owner, mine)
            request_ref[target, 0, 0] = jnp.where(is_far, within + 1, 0)
    first_ref[:, :HD] = k_first[0]
    first_ref[:, HD:] = v_first[0]
    tail_ref[:, :, :HD] = k_tail[...]
    tail_ref[:, :, HD:] = v_tail[...]


def prepare(count, me, block_index, block_count, keys, values):
    qblocks = keys.shape[0]
    entries = block_index.shape[0] * block_index.shape[1]
    first = pl.BlockSpec((1, BLK, HD), lambda i, *_: (0, 0, 0))
    tail = pl.BlockSpec((2, BLK, HD), lambda i, *_: (qblocks // 2 - 1, 0, 0))
    smem = pl.BlockSpec(memory_space=pltpu.SMEM)
    out = (
        jax.ShapeDtypeStruct((count, 1, 128), jnp.int32),
        jax.ShapeDtypeStruct((entries,), jnp.int32),
        jax.ShapeDtypeStruct((entries,), jnp.int32),
        jax.ShapeDtypeStruct((BLK, 2 * HD), BF16),
        jax.ShapeDtypeStruct((2, BLK, 2 * HD), BF16),
    )
    return pl.pallas_call(
        functools.partial(prepare_kernel, count),
        out_shape=out,
        grid_spec=pltpu.PrefetchScalarGridSpec(
            num_scalar_prefetch=1,
            grid=(1,),
            in_specs=[smem, smem, first, first, tail, tail],
            out_specs=[smem, smem, smem, whole(out[3].shape), whole(out[4].shape)],
        ),
        name="prepare",
    )(me, block_index, block_count, keys, values, keys, values)


def serve_kernel(count, chunk, me, asked, k_ref, v_ref, first_ref, out_ref):
    base = pl.program_id(0) * chunk

    @pl.when(me[0] != count - 1)
    def _():
        for d in range(chunk):
            w = jnp.maximum(asked[base + d, 0, 0] - 1, 0)
            out_ref[d, :, :HD] = k_ref[w]
            out_ref[d, :, HD:] = v_ref[w]

    @pl.when(me[0] == count - 1)
    def _():
        for d in range(chunk):
            out_ref[d] = first_ref[...]


def serve(me, asked, keys, values, first):
    count = asked.shape[0]
    chunk = count // 4
    return pl.pallas_call(
        functools.partial(serve_kernel, count, chunk),
        out_shape=jax.ShapeDtypeStruct((count, BLK, 2 * HD), BF16),
        grid_spec=pltpu.PrefetchScalarGridSpec(
            num_scalar_prefetch=1,
            grid=(count // chunk,),
            in_specs=[
                pl.BlockSpec(memory_space=pltpu.SMEM),
                whole(keys.shape), whole(values.shape), whole(first.shape),
            ],
            out_specs=pl.BlockSpec((chunk, BLK, 2 * HD), lambda i, *_: (i, 0, 0)),
        ),
        name="serve",
    )(me, asked, keys, values, first)


def attn_kernel(
    qblocks, max_blocks, far_count, unroll,
    pos, live, order,
    q_ref, o_ref, k_ref, v_ref, prev_ref, far_ref, *rest,
):
    pieces, rest = rest[:qblocks], rest[qblocks:]
    dq_ref, own_ref, dprev_ref, dfar_ref, kv_all, acc, do_all, sems = rest[:8]
    per_row = rest[8:]
    step = pl.program_id(0)
    base = qblocks + 2
    slots = base + far_count
    width = GROUP * BLK

    @pl.when(step == 0)
    def _():
        copies = [
            pltpu.make_async_copy(far_ref, kv_all.at[base:], sems.at[0]),
            pltpu.make_async_copy(prev_ref, kv_all.at[qblocks:base], sems.at[1]),
            pltpu.make_async_copy(k_ref, kv_all.at[:qblocks, :, :HD], sems.at[2]),
            pltpu.make_async_copy(v_ref, kv_all.at[:qblocks, :, HD:], sems.at[3]),
        ]
        for k, piece in enumerate(pieces):
            copies.append(
                pltpu.make_async_copy(piece, do_all.at[order[k]], sems.at[4 + k])
            )
        for copy in copies:
            copy.start()

        def clear(d, carry):
            acc[d] = jnp.zeros((BLK, 2 * HD), F32)
            return carry

        lax.fori_loop(0, slots, clear, 0)
        for copy in copies:
            copy.wait()

    def load(u):
        qs, ds, kg, vg, s_buf, dp_buf, _, _ = per_row[8 * u:8 * u + 8]
        row = step * unroll + u
        mine = slice(u * BLK, (u + 1) * BLK)
        for g in range(GROUP):
            cols = slice(g * HD, (g + 1) * HD)
            qs[g * BLK:(g + 1) * BLK] = q_ref[mine, cols]
            ds[g * BLK:(g + 1) * BLK] = do_all[row, :, cols]
        for e in range(max_blocks):
            p = pos[row * max_blocks + e]
            kg[e * BLK:(e + 1) * BLK] = kv_all[p, :, :HD]
            vg[e * BLK:(e + 1) * BLK] = kv_all[p, :, HD:]
        s_buf[...] = dot(kg[...], qs[...], ((1,), (1,)))
        dp_buf[...] = dot(vg[...], ds[...], ((1,), (1,)))
        ones = jnp.ones((8, 2 * HD), BF16)
        parts = []
        for g in range(GROUP):
            cols = slice(g * HD, (g + 1) * HD)
            prod = ds[g * BLK:(g + 1) * BLK].astype(F32) * o_ref[mine, cols].astype(F32)
            high = prod.astype(BF16)
            low = (prod - high.astype(F32)).astype(BF16)
            parts.append(dot(ones, jnp.concatenate([high, low], axis=1), ((1,), (1,))))
        return jnp.concatenate(parts, axis=1)[0:1]

    def soften(u, out_dot):
        _, _, _, _, s_buf, dp_buf, pt, dst = per_row[8 * u:8 * u + 8]
        row = step * unroll + u
        key_at = lax.broadcasted_iota(jnp.int32, (BLK, width), 0)
        query_at = lax.broadcasted_iota(jnp.int32, (BLK, width), 1) % BLK
        s_buf[:BLK] = jnp.where(key_at <= query_at, s_buf[:BLK], -jnp.inf)
        top = None
        for e in range(max_blocks):
            part = s_buf[e * BLK:(e + 1) * BLK].reshape(BLK // 8, 8, width).max(axis=0)
            if e:
                part = jnp.where(live[row * max_blocks + e] > 0, part, -jnp.inf)
            top = part if top is None else jnp.maximum(top, part)
        shift = top.max(axis=0, keepdims=True) * (SCALE * LOG2E)
        total = None
        for e in range(max_blocks):
            rows = slice(e * BLK, (e + 1) * BLK)
            this = shift
            if e:
                this = jnp.where(live[row * max_blocks + e] > 0, shift, jnp.inf)
            value = jnp.exp2(s_buf[rows] * (SCALE * LOG2E) - this)
            s_buf[rows] = value
            part = value.reshape(BLK // 8, 8, width).sum(axis=0)
            total = part if total is None else total + part
        inverse = 1.0 / total.sum(axis=0, keepdims=True)
        for e in range(max_blocks):
            rows = slice(e * BLK, (e + 1) * BLK)
            probs = s_buf[rows] * inverse
            pt[rows] = probs.astype(BF16)
            dst[rows] = (probs * (dp_buf[rows] - out_dot)).astype(BF16)

    def spread(u):
        qs, ds, kg, _, _, _, pt, dst = per_row[8 * u:8 * u + 8]
        row = step * unroll + u
        dv = dot(pt[...], ds[...], ((1,), (0,)))
        dk = dot(dst[...], qs[...], ((1,), (0,))) * SCALE
        for e in range(max_blocks):
            rows = slice(e * BLK, (e + 1) * BLK)
            p = pos[row * max_blocks + e]
            acc[p, :, :HD] += dk[rows]
            acc[p, :, HD:] += dv[rows]
        dqt = dot(kg[...], dst[...], ((0,), (0,))) * SCALE
        for g in range(GROUP):
            cols = slice(g * HD, (g + 1) * HD)
            dq_ref[u * BLK:(u + 1) * BLK, cols] = dqt[:, cols].T.astype(BF16)

    dots = [load(u) for u in range(unroll)]
    for u in range(unroll):
        soften(u, dots[u])
        spread(u)

    @pl.when(step == qblocks // unroll - 1)
    def _():
        own_ref[...] = acc[:qblocks]
        dprev_ref[...] = acc[qblocks:base].astype(BF16)

        def put(d, carry):
            dfar_ref[d] = acc[base + d].astype(BF16)
            return carry

        lax.fori_loop(0, far_count, put, 0)


def attention(pos, live, order, q, o, keys, values, prev, far, pieces, unroll=1):
    qblocks, far_count = keys.shape[0], far.shape[0]
    max_blocks = pos.shape[0] // qblocks
    slots = qblocks + 2 + far_count
    nkeys = max_blocks * BLK
    width = GROUP * BLK
    out_shapes = (
        jax.ShapeDtypeStruct(q.shape, BF16),
        jax.ShapeDtypeStruct((qblocks, BLK, 2 * HD), F32),
        jax.ShapeDtypeStruct((2, BLK, 2 * HD), BF16),
        jax.ShapeDtypeStruct((far_count, BLK, 2 * HD), BF16),
    )
    rows = pl.BlockSpec((unroll * BLK, width), lambda i, *_: (i, 0))
    anywhere = pl.BlockSpec(memory_space=pl.ANY)
    per_row = [
        pltpu.VMEM((width, HD), BF16),
        pltpu.VMEM((width, HD), BF16),
        pltpu.VMEM((nkeys, HD), BF16),
        pltpu.VMEM((nkeys, HD), BF16),
        pltpu.VMEM((nkeys, width), F32),
        pltpu.VMEM((nkeys, width), F32),
        pltpu.VMEM((nkeys, width), BF16),
        pltpu.VMEM((nkeys, width), BF16),
    ]
    return pl.pallas_call(
        functools.partial(attn_kernel, qblocks, max_blocks, far_count, unroll),
        out_shape=out_shapes,
        grid_spec=pltpu.PrefetchScalarGridSpec(
            num_scalar_prefetch=3,
            grid=(qblocks // unroll,),
            in_specs=[rows, rows] + [anywhere] * (4 + qblocks),
            out_specs=[rows] + [whole(s.shape) for s in out_shapes[1:]],
            scratch_shapes=[
                pltpu.VMEM((slots, BLK, 2 * HD), BF16),
                pltpu.VMEM((slots, BLK, 2 * HD), F32),
                pltpu.VMEM((qblocks, BLK, width), BF16),
                pltpu.SemaphoreType.DMA((4 + qblocks,)),
            ] + per_row * unroll,
        ),
        compiler_params=pltpu.CompilerParams(
            dimension_semantics=("arbitrary",), vmem_limit_bytes=52 << 20
        ),
        cost_estimate=pl.CostEstimate(
            flops=10 * nkeys * width * HD * qblocks, bytes_accessed=16 << 20, transcendentals=0
        ),
        name="attention",
    )(pos, live, order, q, o, keys, values, prev, far, *pieces)


def root_sum_kernel(me, far_ref, out_ref, buf, sem):
    @pl.when(me[0] == far_ref.shape[0] - 1)
    def _():
        copy = pltpu.make_async_copy(far_ref, buf, sem)
        copy.start()
        copy.wait()

        def rows(r, carry):
            at = pl.ds(pl.multiple_of(r * 16, 16), 16)
            total = buf[0, at, :].astype(F32)
            for d in range(1, buf.shape[0]):
                total = total + buf[d, at, :].astype(F32)
            out_ref[at, :] = total
            return carry

        lax.fori_loop(0, BLK // 16, rows, 0)


def root_sum(me, far):
    return pl.pallas_call(
        root_sum_kernel,
        out_shape=jax.ShapeDtypeStruct(far.shape[1:], F32),
        grid_spec=pltpu.PrefetchScalarGridSpec(
            num_scalar_prefetch=1,
            grid=(1,),
            in_specs=[pl.BlockSpec(memory_space=pl.ANY)],
            out_specs=whole(far.shape[1:]),
            scratch_shapes=[pltpu.VMEM(far.shape, BF16), pltpu.SemaphoreType.DMA],
        ),
        compiler_params=pltpu.CompilerParams(vmem_limit_bytes=8 << 20),
        name="root_sum",
    )(me, far)


def finish_kernel(
    qblocks, far_count, asked, own_ref, prev_ref, far_ref, dk_ref, dv_ref, zero_ref, acc,
):
    acc[...] = own_ref[...]
    acc[qblocks - 2:] += prev_ref[...].astype(F32)

    def step(d, carry):
        w = asked[d, 0, 0]

        @pl.when(w > 0)
        def _():
            acc[w - 1] += far_ref[d].astype(F32)

        return carry

    lax.fori_loop(0, far_count, step, 0)
    zero_ref[...] = acc[0]
    for b in range(qblocks):
        dk_ref[b * BLK:(b + 1) * BLK] = acc[b, :, :HD].astype(BF16)
        dv_ref[b * BLK:(b + 1) * BLK] = acc[b, :, HD:].astype(BF16)


def finish(asked, own, prev, far):
    qblocks, far_count = own.shape[0], far.shape[0]
    out = jax.ShapeDtypeStruct((qblocks * BLK, HD), BF16)
    zero = jax.ShapeDtypeStruct((BLK, 2 * HD), F32)
    return pl.pallas_call(
        functools.partial(finish_kernel, qblocks, far_count),
        out_shape=(out, out, zero),
        grid_spec=pltpu.PrefetchScalarGridSpec(
            num_scalar_prefetch=0,
            grid=(1,),
            in_specs=[pl.BlockSpec(memory_space=pltpu.SMEM), whole(own.shape), whole(prev.shape), whole(far.shape)],
            out_specs=[whole(out.shape), whole(out.shape), whole(zero.shape)],
            scratch_shapes=[pltpu.VMEM(own.shape, F32)],
        ),
        compiler_params=pltpu.CompilerParams(vmem_limit_bytes=24 << 20),
        cost_estimate=pl.CostEstimate(
            flops=1 << 30, bytes_accessed=8 << 20, transcendentals=0
        ),
        name="finish",
    )(asked, own, prev, far)


def add_first_kernel(me, first_ref, zero_ref, dk_in, dv_in, dk_ref, dv_ref):
    del dk_in, dv_in
    extra = jnp.where(me[0] == 0, first_ref[...], 0.0)
    total = zero_ref[...] + extra
    dk_ref[...] = total[:, :HD].astype(BF16)
    dv_ref[...] = total[:, HD:].astype(BF16)


def add_first(me, first, zero, dk, dv):
    block = pl.BlockSpec((BLK, HD), lambda i, *_: (0, 0))
    anywhere = pl.BlockSpec(memory_space=pl.ANY)
    return pl.pallas_call(
        add_first_kernel,
        out_shape=(
            jax.ShapeDtypeStruct(dk.shape, BF16), jax.ShapeDtypeStruct(dv.shape, BF16)
        ),
        grid_spec=pltpu.PrefetchScalarGridSpec(
            num_scalar_prefetch=1,
            grid=(1,),
            in_specs=[whole(first.shape), whole(zero.shape), anywhere, anywhere],
            out_specs=[block, block],
        ),
        input_output_aliases={3: 0, 4: 1},
        compiler_params=pltpu.CompilerParams(vmem_limit_bytes=4 << 20),
        name="add_first",
    )(me, first, zero, dk, dv)


def local(query_rows, key_rows, value_rows, attn_out, out_grad, block_index, block_count):
    count = lax.axis_size("seq")
    me = lax.axis_index("seq").astype(jnp.int32).reshape(1)
    heads = lax.axis_size("head")
    my_head = lax.axis_index("head")
    qblocks = key_rows.shape[0] // BLK
    keys = key_rows.reshape(qblocks, BLK, HD)
    values = value_rows.reshape(qblocks, BLK, HD)
    request, position, live, first, tail = prepare(
        count, me, block_index, block_count, keys, values
    )

    first = lax.ppermute(first, "seq", [(0, count - 1)])
    asked = lax.all_to_all(request, "seq", split_axis=0, concat_axis=0, tiled=True)
    prev = lax.ppermute(tail, "seq", [(s, s + 1) for s in range(count - 1)])
    asked, first, prev = lax.optimization_barrier((asked, first, prev))
    served = serve(me, asked, keys, values, first)
    far = lax.all_to_all(served, "seq", split_axis=0, concat_axis=0, tiled=True)

    width = out_grad.shape[1] // heads
    pieces = []
    for k in range(heads):
        piece = lax.dynamic_slice_in_dim(out_grad, ((my_head + k) % heads) * width, width, 1)
        if k:
            piece = lax.ppermute(piece, "head", [(h, (h + k) % heads) for h in range(heads)])
        pieces.append(piece)
    order = (my_head - jnp.arange(heads, dtype=jnp.int32)) % heads

    dq, own, dprev, dfar = attention(
        position, live, order,
        query_rows, attn_out, keys, values, prev, far, pieces,
    )

    prev_back = lax.ppermute(dprev, "seq", [(s + 1, s) for s in range(count - 1)])
    far_back = lax.all_to_all(dfar, "seq", split_axis=0, concat_axis=0, tiled=True)
    first_back = lax.ppermute(root_sum(me, far_back), "seq", [(count - 1, 0)])
    dk, dv, zero = finish(asked, own, prev_back, far_back)
    dk, dv = add_first(me, first_back, zero, dk, dv)
    return dq, dk, dv


def solution(mesh):
    return jax.shard_map(
        local,
        mesh=mesh,
        in_specs=(
            P("seq", "head"),
            P("seq", "head"),
            P("seq", "head"),
            P("seq", "head"),
            P(("seq", "head"), None),
            P("seq", None),
            P("seq"),
        ),
        out_specs=(P("seq", "head"), P("seq", "head"), P("seq", "head")),
        check_vma=False,
    )
```

```python
import functools

import jax
import jax.numpy as jnp
from jax import lax
from jax.experimental import pallas as pl
from jax.experimental.pallas import tpu as pltpu
from jax.sharding import PartitionSpec as P


HD = 128
GROUP = 4
BLK = 128
SCALE = HD ** (-0.5)
LOG2E = 1.4426950408889634
NEAR = 3
ATTN_MIB = 52
F32 = jnp.float32
BF16 = jnp.bfloat16


def dot(a, b, dims):
    return lax.dot_general(a, b, (dims, ((), ())), preferred_element_type=F32)


def whole(shape):
    return pl.BlockSpec(shape, lambda i, *_: (0,) * len(shape))


def prepare_kernel(
    count, me, index_ref, live_count_ref, k_first, v_first, k_tail, v_tail,
    request_ref, pos_ref, live_ref, acc_ref, far_ref, first_ref, tail_ref,
):
    qblocks, max_blocks = index_ref.shape
    mine = me[0]
    shift = qblocks.bit_length() - 1
    assert qblocks == 1 << shift
    for d in range(count):
        request_ref[d, 0, 0] = 0
    for r in range(qblocks):
        front = jnp.int32(0)
        back = jnp.int32(max_blocks - 1)
        for e in range(max_blocks):
            block = index_ref[r, e]
            owner = lax.shift_right_logical(block, shift)
            within = block & (qblocks - 1)
            live = e < live_count_ref[r]
            is_local = owner == mine
            is_prev = (owner == mine - 1) & (within >= qblocks - 2)
            is_near = is_local | is_prev
            is_first = (block == 0) & ~is_near
            is_far = live & ~is_near & ~is_first
            slot = jnp.where(is_first, count - 1, owner)
            near_slot = jnp.where(is_local, within, within + 2)
            at = r * max_blocks + jnp.where(is_near, front, back)
            pos_ref[at] = jnp.where(is_near, near_slot, slot + (qblocks + 2))
            live_ref[at] = live.astype(jnp.int32)
            acc_ref[at] = jnp.where(
                is_near, near_slot, jnp.where(is_first, qblocks + 2, qblocks + 3)
            )
            far_ref[at] = jnp.where(is_far, owner, mine)
            front = front + is_near.astype(jnp.int32)
            back = back - 1 + is_near.astype(jnp.int32)
            target = jnp.where(is_far, owner, mine)
            request_ref[target, 0, 0] = jnp.where(is_far, within + 1, 0)
    first_ref[:, :HD] = k_first[0]
    first_ref[:, HD:] = v_first[0]
    tail_ref[:, :, :HD] = k_tail[...]
    tail_ref[:, :, HD:] = v_tail[...]


def prepare(count, me, block_index, block_count, keys, values):
    qblocks = keys.shape[0]
    entries = block_index.shape[0] * block_index.shape[1]
    first = pl.BlockSpec((1, BLK, HD), lambda i, *_: (0, 0, 0))
    tail = pl.BlockSpec((2, BLK, HD), lambda i, *_: (qblocks // 2 - 1, 0, 0))
    smem = pl.BlockSpec(memory_space=pltpu.SMEM)
    table = jax.ShapeDtypeStruct((entries,), jnp.int32)
    out = (
        jax.ShapeDtypeStruct((count, 1, 128), jnp.int32),
        table, table, table, table,
        jax.ShapeDtypeStruct((BLK, 2 * HD), BF16),
        jax.ShapeDtypeStruct((2, BLK, 2 * HD), BF16),
    )
    return pl.pallas_call(
        functools.partial(prepare_kernel, count),
        out_shape=out,
        grid_spec=pltpu.PrefetchScalarGridSpec(
            num_scalar_prefetch=1,
            grid=(1,),
            in_specs=[smem, smem, first, first, tail, tail],
            out_specs=[smem] * 5 + [whole(out[5].shape), whole(out[6].shape)],
        ),
        name="prepare",
    )(me, block_index, block_count, keys, values, keys, values)


def serve_kernel(count, chunk, me, asked, k_ref, v_ref, first_ref, out_ref):
    base = pl.program_id(0) * chunk

    @pl.when(me[0] != count - 1)
    def _():
        for d in range(chunk):
            w = jnp.maximum(asked[base + d, 0, 0] - 1, 0)
            out_ref[d, :, :HD] = k_ref[w]
            out_ref[d, :, HD:] = v_ref[w]

    @pl.when(me[0] == count - 1)
    def _():
        for d in range(chunk):
            out_ref[d] = first_ref[...]


def serve(me, asked, keys, values, first):
    count = asked.shape[0]
    chunk = count // 4
    return pl.pallas_call(
        functools.partial(serve_kernel, count, chunk),
        out_shape=jax.ShapeDtypeStruct((count, BLK, 2 * HD), BF16),
        grid_spec=pltpu.PrefetchScalarGridSpec(
            num_scalar_prefetch=1,
            grid=(count // chunk,),
            in_specs=[
                pl.BlockSpec(memory_space=pltpu.SMEM),
                whole(keys.shape), whole(values.shape), whole(first.shape),
            ],
            out_specs=pl.BlockSpec((chunk, BLK, 2 * HD), lambda i, *_: (i, 0, 0)),
        ),
        name="serve",
    )(me, asked, keys, values, first)


def gather_heads(dst, src):
    for g in range(GROUP):
        dst[g * BLK:(g + 1) * BLK] = src[:, g * HD:(g + 1) * HD]


def attn_kernel(
    qblocks, max_blocks, far_count,
    pos, live, acc_at, far_at, order,
    q_ref, o_ref, k_ref, v_ref, prev_ref, far_ref, *rest,
):
    pieces, rest = rest[:qblocks], rest[qblocks:]
    dfar_ref, sums_ref, pt_near, dst_ref, kg_ref = rest[:5]
    kv_all, acc, do_all, qs, ds, vg, s_buf, dp_buf, pt_flex, stats, sems = rest[5:]
    kg = kg_ref.at[0]
    row = pl.program_id(0)
    base = qblocks + 2
    width = GROUP * BLK
    near = NEAR * BLK
    dst = dst_ref.at[0]

    @pl.when(row == 0)
    def _():
        copies = [
            pltpu.make_async_copy(far_ref, kv_all.at[base:], sems.at[0]),
            pltpu.make_async_copy(prev_ref, kv_all.at[qblocks:base], sems.at[1]),
            pltpu.make_async_copy(k_ref, kv_all.at[:qblocks, :, :HD], sems.at[2]),
            pltpu.make_async_copy(v_ref, kv_all.at[:qblocks, :, HD:], sems.at[3]),
        ]
        for k, piece in enumerate(pieces):
            copies.append(
                pltpu.make_async_copy(piece, do_all.at[order[k]], sems.at[4 + k])
            )
        for copy in copies:
            copy.start()

        def clear(d, carry):
            acc[d] = jnp.zeros((BLK, 2 * HD), F32)
            return carry

        lax.fori_loop(0, acc.shape[0], clear, 0)
        for copy in copies:
            copy.wait()

    def stage(body):
        pl.when(row >= 0)(body)

    @stage
    def _():
        gather_heads(qs, q_ref)
        gather_heads(ds, do_all.at[row])
        for e in range(max_blocks):
            p = pos[row * max_blocks + e]
            kg[e * BLK:(e + 1) * BLK] = kv_all[p, :, :HD]
            vg[e * BLK:(e + 1) * BLK] = kv_all[p, :, HD:]

    @stage
    def _():
        s_buf[...] = dot(kg[...], qs[...], ((1,), (1,)))
        ones = jnp.ones((8, 2 * HD), BF16)
        for g in range(GROUP):
            cols = slice(g * HD, (g + 1) * HD)
            prod = ds[g * BLK:(g + 1) * BLK].astype(F32) * o_ref[:, cols].astype(F32)
            high = prod.astype(BF16)
            low = (prod - high.astype(F32)).astype(BF16)
            both = jnp.concatenate([high, low], axis=1)
            stats[0, :, cols] = dot(ones, both, ((1,), (1,)))

    @stage
    def _():
        key_at = lax.broadcasted_iota(jnp.int32, (BLK, width), 0)
        query_at = lax.broadcasted_iota(jnp.int32, (BLK, width), 1) % BLK
        top = None
        for e in range(max_blocks):
            part = s_buf[e * BLK:(e + 1) * BLK]
            if e == 0:
                part = jnp.where(key_at <= query_at, part, -jnp.inf)
                s_buf[:BLK] = part
            part = part.reshape(BLK // 8, 8, width).max(axis=0)
            if e:
                part = jnp.where(live[row * max_blocks + e] > 0, part, -jnp.inf)
            top = part if top is None else jnp.maximum(top, part)
        top = top.max(axis=0, keepdims=True) * (SCALE * LOG2E)
        stats[1] = jnp.broadcast_to(top, (8, width))

    @stage
    def _():
        dp_buf[...] = dot(vg[...], ds[...], ((1,), (1,)))
        shift = stats[1]
        total = None
        for e in range(max_blocks):
            rows = slice(e * BLK, (e + 1) * BLK)
            this = shift
            if e:
                this = jnp.where(live[row * max_blocks + e] > 0, shift, jnp.inf)
            tile = s_buf[rows].reshape(BLK // 8, 8, width)
            value = jnp.exp2(tile * (SCALE * LOG2E) - this[None])
            s_buf[rows] = value.reshape(BLK, width)
            part = value.sum(axis=0)
            total = part if total is None else total + part
        total = 1.0 / total.sum(axis=0, keepdims=True)
        stats[2] = jnp.broadcast_to(total, (8, width))

    @stage
    def _():
        out_dot = stats[0]
        inverse = stats[2]
        for e in range(max_blocks):
            rows = slice(e * BLK, (e + 1) * BLK)
            probs = s_buf[rows].reshape(BLK // 8, 8, width) * inverse[None]
            grads = probs * (dp_buf[rows].reshape(BLK // 8, 8, width) - out_dot[None])
            probs = probs.reshape(BLK, width).astype(BF16)
            if e < NEAR:
                pt_near[0, rows] = probs
            else:
                pt_flex[(e - NEAR) * BLK:(e - NEAR + 1) * BLK] = probs
            dst[rows] = grads.reshape(BLK, width).astype(BF16)

    @stage
    def _():
        dv = dot(pt_flex[...], ds[...], ((1,), (0,)))
        dk = dot(dst[near:], qs[...], ((1,), (0,))) * SCALE
        for e in range(NEAR, max_blocks):
            rows = slice((e - NEAR) * BLK, (e - NEAR + 1) * BLK)
            a = acc_at[row * max_blocks + e]
            f = far_at[row * max_blocks + e]
            acc[a, :, :HD] += dk[rows]
            acc[a, :, HD:] += dv[rows]
            dfar_ref[f, :, :HD] = dk[rows].astype(BF16)
            dfar_ref[f, :, HD:] = dv[rows].astype(BF16)

    @pl.when(row == qblocks - 1)
    def _():
        sums_ref[...] = acc[:base]
        dfar_ref[far_count - 1] = acc[base].astype(BF16)


def scratch_of(shape, dtype=BF16):
    return pltpu.VMEM(shape, dtype)


def attention(tables, order, q, o, keys, values, prev, far, pieces):
    qblocks, far_count = keys.shape[0], far.shape[0]
    max_blocks = tables[0].shape[0] // qblocks
    base = qblocks + 2
    nkeys = max_blocks * BLK
    width = GROUP * BLK
    near = NEAR * BLK
    out_shapes = (
        pltpu.HBM((far_count, BLK, 2 * HD), BF16),
        pltpu.HBM((base, BLK, 2 * HD), F32),
        pltpu.HBM((qblocks, near, width), BF16),
        pltpu.HBM((qblocks, nkeys, width), BF16),
        pltpu.HBM((qblocks, nkeys, HD), BF16),
    )
    rows = pl.BlockSpec((BLK, width), lambda i, *_: (i, 0))
    anywhere = pl.BlockSpec(memory_space=pltpu.HBM)
    return pl.pallas_call(
        functools.partial(attn_kernel, qblocks, max_blocks, far_count),
        out_shape=out_shapes,
        grid_spec=pltpu.PrefetchScalarGridSpec(
            num_scalar_prefetch=5,
            grid=(qblocks,),
            in_specs=[rows, rows] + [anywhere] * 3 + [pl.BlockSpec(memory_space=pl.ANY)] + [anywhere] * qblocks,
            out_specs=[
                whole(out_shapes[0].shape),
                whole(out_shapes[1].shape),
                pl.BlockSpec((1, near, width), lambda i, *_: (i, 0, 0)),
                pl.BlockSpec((1, nkeys, width), lambda i, *_: (i, 0, 0)),
                pl.BlockSpec((1, nkeys, HD), lambda i, *_: (i, 0, 0)),
            ],
            scratch_shapes=[
                scratch_of((base + far_count, BLK, 2 * HD)),
                scratch_of((base + 2, BLK, 2 * HD), F32),
                scratch_of((qblocks, BLK, width)),
                scratch_of((width, HD)),
                scratch_of((width, HD)),
                scratch_of((nkeys, HD)),
                scratch_of((nkeys, width), F32),
                scratch_of((nkeys, width), F32),
                scratch_of((nkeys - near, width)),
                scratch_of((3, 8, width), F32),
                pltpu.SemaphoreType.DMA((4 + qblocks,)),
            ],
        ),
        compiler_params=pltpu.CompilerParams(
            dimension_semantics=("arbitrary",), vmem_limit_bytes=ATTN_MIB << 20
        ),
        cost_estimate=pl.CostEstimate(
            flops=10 * nkeys * width * HD * qblocks, bytes_accessed=16 << 20, transcendentals=0
        ),
        name="attention",
    )(*tables, order, q, o, keys, values, prev, far, *pieces)


def rest_kernel(
    qblocks, max_blocks,
    acc_at, order,
    q_ref, pt_near, dst_ref, kg_ref, sums_ref, *rest,
):
    pieces, rest = rest[:qblocks], rest[qblocks:]
    dq_ref, own_ref, dprev_ref, acc, do_all, qs, ds, sems = rest
    row = pl.program_id(0)

    @pl.when(row == 0)
    def _():
        copies = [
            pltpu.make_async_copy(sums_ref, acc, sems.at[qblocks]),
        ]
        for k, piece in enumerate(pieces):
            copies.append(
                pltpu.make_async_copy(piece, do_all.at[order[k]], sems.at[k])
            )
        for copy in copies:
            copy.start()
        for copy in copies:
            copy.wait()

    gather_heads(qs, q_ref)
    gather_heads(ds, do_all.at[row])
    dv = dot(pt_near[0], ds[...], ((1,), (0,)))
    dk = dot(dst_ref[0, :NEAR * BLK], qs[...], ((1,), (0,))) * SCALE
    for e in range(NEAR):
        rows = slice(e * BLK, (e + 1) * BLK)
        a = acc_at[row * max_blocks + e]
        acc[a, :, :HD] += dk[rows]
        acc[a, :, HD:] += dv[rows]
    dqt = dot(kg_ref[0], dst_ref[0], ((0,), (0,))) * SCALE
    for g in range(GROUP):
        cols = slice(g * HD, (g + 1) * HD)
        dq_ref[:, cols] = dqt[:, cols].T.astype(BF16)

    @pl.when(row == qblocks - 1)
    def _():
        own_ref[...] = acc[:qblocks]
        dprev_ref[...] = acc[qblocks:].astype(BF16)


def rest_of(acc_at, order, q, pt_near, dst, kg, sums, pieces):
    qblocks = len(pieces)
    nkeys = dst.shape[1]
    max_blocks = nkeys // BLK
    base = qblocks + 2
    width = GROUP * BLK
    near = NEAR * BLK
    rows = pl.BlockSpec((BLK, width), lambda i, *_: (i, 0))
    anywhere = pl.BlockSpec(memory_space=pltpu.HBM)
    out_shapes = (
        jax.ShapeDtypeStruct(q.shape, BF16),
        jax.ShapeDtypeStruct((qblocks, BLK, 2 * HD), F32),
        jax.ShapeDtypeStruct((2, BLK, 2 * HD), BF16),
    )
    return pl.pallas_call(
        functools.partial(rest_kernel, qblocks, max_blocks),
        out_shape=out_shapes,
        grid_spec=pltpu.PrefetchScalarGridSpec(
            num_scalar_prefetch=2,
            grid=(qblocks,),
            in_specs=[
                rows,
                pl.BlockSpec((1, near, width), lambda i, *_: (i, 0, 0)),
                pl.BlockSpec((1, nkeys, width), lambda i, *_: (i, 0, 0)),
                pl.BlockSpec((1, nkeys, HD), lambda i, *_: (i, 0, 0)),
            ] + [anywhere] * (1 + qblocks),
            out_specs=[rows, whole(out_shapes[1].shape), whole(out_shapes[2].shape)],
            scratch_shapes=[
                scratch_of((base, BLK, 2 * HD), F32),
                scratch_of((qblocks, BLK, width)),
                scratch_of((width, HD)),
                scratch_of((width, HD)),
                pltpu.SemaphoreType.DMA((1 + qblocks,)),
            ],
        ),
        compiler_params=pltpu.CompilerParams(
            dimension_semantics=("arbitrary",), vmem_limit_bytes=56 << 20
        ),
        cost_estimate=pl.CostEstimate(
            flops=10 * nkeys * width * HD * qblocks, bytes_accessed=16 << 20, transcendentals=0
        ),
        name="rest",
    )(acc_at, order, q, pt_near, dst, kg, sums, *pieces)


def root_sum_kernel(me, far_ref, out_ref, buf, sem):
    @pl.when(me[0] == far_ref.shape[0] - 1)
    def _():
        copy = pltpu.make_async_copy(far_ref, buf, sem)
        copy.start()
        copy.wait()

        def rows(r, carry):
            at = pl.ds(pl.multiple_of(r * 16, 16), 16)
            total = buf[0, at, :].astype(F32)
            for d in range(1, buf.shape[0]):
                total = total + buf[d, at, :].astype(F32)
            out_ref[at, :] = total.astype(BF16)
            return carry

        lax.fori_loop(0, BLK // 16, rows, 0)


def root_sum(me, far):
    return pl.pallas_call(
        root_sum_kernel,
        out_shape=jax.ShapeDtypeStruct(far.shape[1:], BF16),
        grid_spec=pltpu.PrefetchScalarGridSpec(
            num_scalar_prefetch=1,
            grid=(1,),
            in_specs=[pl.BlockSpec(memory_space=pl.ANY)],
            out_specs=whole(far.shape[1:]),
            scratch_shapes=[pltpu.VMEM(far.shape, BF16), pltpu.SemaphoreType.DMA],
        ),
        compiler_params=pltpu.CompilerParams(vmem_limit_bytes=8 << 20),
        name="root_sum",
    )(me, far)


def finish_kernel(
    qblocks, far_count, asked, own_ref, prev_ref, far_ref, dk_ref, dv_ref, zero_ref, acc,
):
    acc[...] = own_ref[...]
    acc[qblocks - 2:] += prev_ref[...].astype(F32)

    def step(d, carry):
        w = asked[d, 0, 0]

        @pl.when(w > 0)
        def _():
            acc[w - 1] += far_ref[d].astype(F32)

        return carry

    lax.fori_loop(0, far_count, step, 0)
    zero_ref[...] = acc[0]
    for b in range(qblocks):
        dk_ref[b * BLK:(b + 1) * BLK] = acc[b, :, :HD].astype(BF16)
        dv_ref[b * BLK:(b + 1) * BLK] = acc[b, :, HD:].astype(BF16)


def finish(asked, own, prev, far):
    qblocks, far_count = own.shape[0], far.shape[0]
    out = jax.ShapeDtypeStruct((qblocks * BLK, HD), BF16)
    zero = jax.ShapeDtypeStruct((BLK, 2 * HD), F32)
    return pl.pallas_call(
        functools.partial(finish_kernel, qblocks, far_count),
        out_shape=(out, out, zero),
        grid_spec=pltpu.PrefetchScalarGridSpec(
            num_scalar_prefetch=0,
            grid=(1,),
            in_specs=[pl.BlockSpec(memory_space=pltpu.SMEM), whole(own.shape), whole(prev.shape), whole(far.shape)],
            out_specs=[whole(out.shape), whole(out.shape), whole(zero.shape)],
            scratch_shapes=[pltpu.VMEM(own.shape, F32)],
        ),
        compiler_params=pltpu.CompilerParams(vmem_limit_bytes=24 << 20),
        cost_estimate=pl.CostEstimate(
            flops=1 << 30, bytes_accessed=8 << 20, transcendentals=0
        ),
        name="finish",
    )(asked, own, prev, far)


def add_first_kernel(me, first_ref, zero_ref, dk_in, dv_in, dk_ref, dv_ref):
    del dk_in, dv_in
    extra = jnp.where(me[0] == 0, first_ref[...].astype(F32), 0.0)
    total = zero_ref[...] + extra
    dk_ref[...] = total[:, :HD].astype(BF16)
    dv_ref[...] = total[:, HD:].astype(BF16)


def add_first(me, first, zero, dk, dv):
    block = pl.BlockSpec((BLK, HD), lambda i, *_: (0, 0))
    anywhere = pl.BlockSpec(memory_space=pl.ANY)
    return pl.pallas_call(
        add_first_kernel,
        out_shape=(
            jax.ShapeDtypeStruct(dk.shape, BF16), jax.ShapeDtypeStruct(dv.shape, BF16)
        ),
        grid_spec=pltpu.PrefetchScalarGridSpec(
            num_scalar_prefetch=1,
            grid=(1,),
            in_specs=[whole(first.shape), whole(zero.shape), anywhere, anywhere],
            out_specs=[block, block],
        ),
        input_output_aliases={3: 0, 4: 1},
        compiler_params=pltpu.CompilerParams(vmem_limit_bytes=4 << 20),
        name="add_first",
    )(me, first, zero, dk, dv)


def local(query_rows, key_rows, value_rows, attn_out, out_grad, block_index, block_count):
    count = lax.axis_size("seq")
    me = lax.axis_index("seq").astype(jnp.int32).reshape(1)
    heads = lax.axis_size("head")
    my_head = lax.axis_index("head")
    qblocks = key_rows.shape[0] // BLK
    keys = key_rows.reshape(qblocks, BLK, HD)
    values = value_rows.reshape(qblocks, BLK, HD)
    request, position, live, acc_at, far_at, first, tail = prepare(
        count, me, block_index, block_count, keys, values
    )

    first = lax.ppermute(first, "seq", [(0, count - 1)])
    asked = lax.all_to_all(request, "seq", split_axis=0, concat_axis=0, tiled=True)
    prev = lax.ppermute(tail, "seq", [(s, s + 1) for s in range(count - 1)])
    asked, first = lax.optimization_barrier((asked, first))
    served = serve(me, asked, keys, values, first)
    far = lax.all_to_all(served, "seq", split_axis=0, concat_axis=0, tiled=True)

    width = out_grad.shape[1] // heads
    pieces = []
    for k in range(heads):
        piece = lax.dynamic_slice_in_dim(out_grad, ((my_head + k) % heads) * width, width, 1)
        if k:
            piece = lax.ppermute(piece, "head", [(h, (h + k) % heads) for h in range(heads)])
        pieces.append(piece)
    order = (my_head - jnp.arange(heads, dtype=jnp.int32)) % heads

    dfar, sums, pt_near, dst, kg = attention(
        (position, live, acc_at, far_at), order,
        query_rows, attn_out, keys, values, prev, far, pieces,
    )
    far_back = lax.all_to_all(dfar, "seq", split_axis=0, concat_axis=0, tiled=True)
    dq, own, dprev = rest_of(
        acc_at, order, query_rows, pt_near, dst, kg, sums, pieces
    )
    prev_back = lax.ppermute(dprev, "seq", [(s + 1, s) for s in range(count - 1)])
    first_back = lax.ppermute(root_sum(me, far_back), "seq", [(count - 1, 0)])
    dk, dv, zero = finish(asked, own, prev_back, far_back)
    dk, dv = add_first(me, first_back, zero, dk, dv)
    return dq, dk, dv


def solution(mesh):
    return jax.shard_map(
        local,
        mesh=mesh,
        in_specs=(
            P("seq", "head"),
            P("seq", "head"),
            P("seq", "head"),
            P("seq", "head"),
            P(("seq", "head"), None),
            P("seq", None),
            P("seq"),
        ),
        out_specs=(P("seq", "head"), P("seq", "head"), P("seq", "head")),
        check_vma=False,
    )
```
